8 devices in a mesh: dp: 1 (over z), tp: 2 (over y), ep: 4 (over x, core).
Axes of the slice: x: 2, y: 2, z: 1, core: 2. Of those that a mesh axis runs over, the one named last changes fastest.
Arguments:
- tokens: bfloat16 [1024, 2304], P(('dp', 'ep', 'tp'))
- expert_ids: int32 [1024, 2], P(('dp', 'ep', 'tp'))
- gates: float32 [1024, 2], P(('dp', 'ep', 'tp'))
- w_gate: bfloat16 [8, 2304, 5760], P('ep', None, 'tp')
- w_up: bfloat16 [8, 2304, 5760], P('ep', None, 'tp')
- w_down: bfloat16 [8, 5760, 2304], P('ep', 'tp')
Outputs:
- output: bfloat16 [1024, 2304], P(('dp', 'ep', 'tp'))
All inputs are finite; a program needn't handle non-finite values.
Results may differ from the reference program's by a relative error of at most 0.001.
Values are sent between devices in bfloat16 or wider.
A program may use at most 1 GiB of HBM per device.

```python
import jax
import jax.numpy as jnp
from jax import lax

TOKENS_DEV = 128
HIDDEN = 2304
EXPERT_FF = 5760
EXPERTS = 8
TOP_K = 2
EP_SIZE = 4
TP_SIZE = 2

TOKENS = TOKENS_DEV * EP_SIZE * TP_SIZE
SPREAD = min(TOP_K, EP_SIZE)


def routing_ids(base_key):
    group_devices = EP_SIZE * TP_SIZE
    class_rows = TOKENS_DEV // EP_SIZE
    local_count = EXPERTS // EP_SIZE
    key_rows, key_target, key_rot = jax.random.split(base_key, 3)
    row_order = jax.vmap(lambda sub_key: jax.random.permutation(sub_key, TOKENS_DEV))(jax.random.split(key_rows, group_devices))
    ep_order = jax.vmap(lambda sub_key: jax.random.permutation(sub_key, EP_SIZE))(jax.random.split(key_target, group_devices))
    rotation = jax.random.randint(key_rot, (), 0, local_count)
    slots = jnp.arange(TOP_K)
    ep_class = row_order % EP_SIZE
    within = row_order // EP_SIZE + jnp.arange(group_devices)[:, None] * class_rows
    place = (ep_class[:, :, None] + slots % SPREAD) % EP_SIZE
    target_ep = jax.vmap(lambda order_row, place_rows: order_row[place_rows])(ep_order, place)
    local_slot = (within[:, :, None] + slots // SPREAD + rotation) % local_count
    return (target_ep * local_count + local_slot).astype(jnp.int32).reshape(TOKENS, TOP_K)


def setup_inputs(seed: int = 0, part: int = 0) -> dict:
    base_key = jax.random.key(seed)
    key_gate_w, key_up_w, key_down_w, key_part = jax.random.split(base_key, 4)
    key_tokens, key_ids, key_gates = jax.random.split(jax.random.fold_in(key_part, part), 3)
    tokens = jax.random.normal(key_tokens, (TOKENS, HIDDEN), jnp.float32).astype(jnp.bfloat16)
    expert_ids = routing_ids(key_ids)
    gates = jax.random.uniform(key_gates, (TOKENS, TOP_K), jnp.float32, 0.5, 1.5)
    w_gate = (jax.random.normal(key_gate_w, (EXPERTS, HIDDEN, EXPERT_FF), jnp.float32) * HIDDEN ** -0.5).astype(jnp.bfloat16)
    w_up = (jax.random.normal(key_up_w, (EXPERTS, HIDDEN, EXPERT_FF), jnp.float32) * HIDDEN ** -0.5).astype(jnp.bfloat16)
    w_down = (jax.random.normal(key_down_w, (EXPERTS, EXPERT_FF, HIDDEN), jnp.float32) * EXPERT_FF ** -0.5).astype(jnp.bfloat16)
    return {"tokens": tokens, "expert_ids": expert_ids, "gates": gates, "w_gate": w_gate, "w_up": w_up, "w_down": w_down}


def reference(tokens, expert_ids, gates, w_gate, w_up, w_down):
    load = TOKENS * TOP_K // EXPERTS
    order = jnp.argsort(expert_ids.reshape(-1), stable=True).reshape(EXPERTS, load)
    row_index = order // TOP_K
    gate_sorted = gates.reshape(-1)[order]

    def expert_out(operands):
        rows_in, gate_in, gate_mat, up_mat, down_mat = operands
        x_rows = tokens[rows_in]
        hidden_gate = jnp.dot(x_rows, gate_mat, preferred_element_type=jnp.float32)
        hidden_up = jnp.dot(x_rows, up_mat, preferred_element_type=jnp.float32)
        act_rows = (jax.nn.silu(hidden_gate) * hidden_up).astype(jnp.bfloat16)
        out_rows = jnp.dot(act_rows, down_mat, preferred_element_type=jnp.float32)
        return out_rows * gate_in[:, None]

    weighted = lax.map(expert_out, (row_index, gate_sorted, w_gate, w_up, w_down))
    summed = jax.ops.segment_sum(weighted.reshape(-1, HIDDEN), row_index.reshape(-1), num_segments=TOKENS)
    return summed.astype(jnp.bfloat16)
```

```python
import functools

import jax
import jax.numpy as jnp
from jax import lax
from jax.experimental import pallas as pl
from jax.experimental.pallas import tpu as pltpu
from jax.sharding import PartitionSpec as P

MESH = pl.DeviceIdType.MESH
F32 = jnp.float32
BF16 = jnp.bfloat16

ROWS = 128
SLOTS = 64
KC = 256
CC = 256
WRING = 3
DRING = 2
LAG1, LAG2 = 1, 2


def f32dot(a, b):
    return jnp.dot(a, b, preferred_element_type=F32)


def split3(v):
    hi = v.astype(BF16)
    rest = v - hi.astype(F32)
    mid = rest.astype(BF16)
    low = (rest - mid.astype(F32)).astype(BF16)
    return jnp.concatenate([hi, mid, low], axis=1)


def sum3(v):
    n = v.shape[1] // 3
    return (v[:, 2 * n:] + v[:, n:2 * n]) + v[:, :n]


def chunks(total, size):
    return [(i, min(size, total - i)) for i in range(0, total, size)]


def kernel(meta_ref, tok_ref, wg_hbm, wu_hbm, wd_hbm, y_ref,
           meta_all, pack, slots, xs, wg_buf, wu_buf, wd_buf, acc_g, acc_u, h,
           perm, perm_t, merge, gcol, parts, o_a, o_b,
           a1, a2s, a2, b1, b2s, b2, own_b,
           meta_ss, meta_rs, d_ss, d_rs, w_sem, wd_sem,
           a1_ss, a1_rs, a2_ss, a2_rs, b1_ss, b1_rs, b2_ss, b2_rs):
    ep, tp = lax.axis_index("ep"), lax.axis_index("tp")
    core, x = lax.rem(ep, 2), lax.div(ep, 2)
    nk, ns = slots.shape[0], o_b.shape[0]
    ff = wg_buf.shape[3]

    def peer(rel):
        dx, dc, dy = rel // 4, (rel // 2) % 2, rel % 2
        return {"ep": lax.rem(x + dx, 2) * 2 + lax.rem(core + dc, 2), "tp": lax.rem(tp + dy, 2)}

    def ep_of(k):
        return lax.rem(x + k // 2, 2) * 2 + lax.rem(core + k % 2, 2)

    def w_copies(kc, slot):
        at = pl.ds(pl.multiple_of(kc * KC, KC), KC)
        return (pltpu.make_async_copy(wg_hbm.at[:, at, :], wg_buf.at[slot], w_sem.at[0, slot]),
                pltpu.make_async_copy(wu_hbm.at[:, at, :], wu_buf.at[slot], w_sem.at[1, slot]))

    def wd_copy(s, slot):
        at = pl.ds(pl.multiple_of(s * CC, CC), CC)
        return pltpu.make_async_copy(wd_hbm.at[:, :, at], wd_buf.at[slot], wd_sem.at[slot])

    def remote(src, dst, ss, rs, rel):
        return pltpu.make_async_remote_copy(src_ref=src, dst_ref=dst, send_sem=ss, recv_sem=rs,
                                            device_id=peer(rel), device_id_type=MESH)

    for i in range(WRING):
        for c in w_copies(i, i):
            c.start()
    for i in range(DRING):
        wd_copy(i, i).start()

    barrier = pltpu.get_barrier_semaphore()
    for rel in range(1, 8):
        pl.semaphore_signal(barrier, inc=1, device_id=peer(rel), device_id_type=MESH)
    pl.semaphore_wait(barrier, 7)

    def meta_copy(rel):
        return remote(meta_ref, meta_all.at[rel], meta_ss.at[rel], meta_rs.at[rel], rel)

    for rel in range(1, 8):
        meta_copy(rel).start()

    sub128 = lax.broadcasted_iota(jnp.int32, (ROWS, ROWS), 0)
    lane128 = lax.broadcasted_iota(jnp.int32, (ROWS, ROWS), 1)
    before = jnp.where(sub128 < lane128, 1.0, 0.0).astype(BF16)

    def select(meta, epv):
        lo = 2.0 * epv.astype(F32)
        id0, id1, g0, g1 = (meta[i:i + 1, :] for i in range(4))
        first = (id0 >= lo) & (id0 <= lo + 1.0)
        second = (id1 >= lo) & (id1 <= lo + 1.0)
        mask = jnp.where(first | second, 1.0, 0.0)
        local = jnp.where(first, id0 - lo, jnp.where(second, id1 - lo, 0.0))
        gate = jnp.where(first, g0, jnp.where(second, g1, 0.0))
        return mask, local, gate

    def ranks(masks):
        m = jnp.concatenate(masks + masks[:1] * (8 - len(masks)), axis=0)
        r = f32dot(m.astype(BF16), before)
        return jnp.where(m > 0.5, r, -1.0)

    slot_iota = lax.broadcasted_iota(jnp.int32, (SLOTS, ROWS), 0).astype(F32)
    own = ranks([select(meta_ref[...], ep_of(k))[0] for k in range(4)])
    pick = jnp.concatenate(
        [jnp.where(own[k:k + 1, :] == slot_iota, 1.0, 0.0) for k in range(4)], axis=0).astype(BF16)

    def d_copy(kc, rel):
        k = rel // 2
        return remote(pack.at[kc, pl.ds(k * SLOTS, SLOTS)], slots.at[kc, pl.ds(rel * SLOTS, SLOTS)],
                      d_ss.at[kc, rel], d_rs.at[kc, rel], rel)

    for kc in range(nk):
        pack[kc] = f32dot(pick, tok_ref[:, kc * KC:(kc + 1) * KC]).astype(BF16)
        slots[kc, 0:SLOTS] = pack[kc, 0:SLOTS]
        for rel in (7, 4, 5, 6, 1, 3, 2):
            d_copy(kc, rel).start()

    acc_g[...] = jnp.zeros_like(acc_g)
    acc_u[...] = jnp.zeros_like(acc_u)

    for rel in range(1, 8):
        meta_copy(rel).wait()
    meta_all[0] = meta_ref[...]

    chosen = [select(meta_all[rel], ep) for rel in range(8)]
    rank_in = ranks([c[0] for c in chosen])
    local_cols = []
    for rel in range(8):
        hit = rank_in[rel:rel + 1, :] == slot_iota
        local_cols.append(jnp.sum(jnp.where(hit, chosen[rel][1], 0.0), axis=1, keepdims=True))
        gcol[rel * SLOTS:(rel + 1) * SLOTS, :] = jnp.broadcast_to(
            jnp.sum(jnp.where(hit, chosen[rel][2], 0.0), axis=1, keepdims=True), (SLOTS, ROWS))
    nq = 8 * SLOTS
    local = jnp.concatenate([jnp.broadcast_to(c, (SLOTS, ROWS)) for c in local_cols], axis=0)
    q_sub = lax.broadcasted_iota(jnp.int32, (nq, nq), 0)
    q_lane = lax.broadcasted_iota(jnp.int32, (nq, nq), 1)
    after = jnp.where(q_sub > q_lane, 1.0, 0.0).astype(BF16)
    ones_before = f32dot(after, local.astype(BF16))
    q_col = lax.broadcasted_iota(jnp.int32, (nq, ROWS), 0).astype(F32)
    l_row = lax.broadcasted_iota(jnp.int32, (nq, ROWS), 1).astype(F32)
    place = jnp.where(local > 0.5, nq // 2 + ones_before, q_col - ones_before)
    diag = sub128 == lane128
    for j in range(nq // ROWS):
        at = slice(j * ROWS, (j + 1) * ROWS)
        perm_t[:, at] = jnp.where(place == l_row + float(j * ROWS), 1.0, 0.0).astype(BF16)
        row = jnp.sum(jnp.where(diag, place[at, :], 0.0), axis=0, keepdims=True)
        perm[:, at] = jnp.where(row == q_col, 1.0, 0.0).astype(BF16)

    s_lane = lane128.astype(F32)
    par = ranks([select(meta_all[1], ep_of(k))[0] for k in range(4)])
    for who, r in enumerate((own, par)):
        cols = [jnp.sum(jnp.where(diag, r[k:k + 1, :], 0.0), axis=1, keepdims=True) for k in range(4)]
        for j in range(2):
            hit = jnp.where(s_lane < float(SLOTS), cols[2 * j] - s_lane,
                            cols[2 * j + 1] - s_lane + float(SLOTS)) == 0.0
            merge[who, :, j * ROWS:(j + 1) * ROWS] = jnp.where(hit, 1.0, 0.0).astype(BF16)

    half = nq // 2

    def arrive(kc):
        slot = lax.rem(kc, WRING)
        for rel in range(1, 8):
            d_copy(kc, rel).wait_recv()
        xs[...] = f32dot(perm[...], slots[kc]).astype(BF16)
        for c in w_copies(kc, slot):
            c.wait()
        return slot

    def k_step(kc, carry):
        slot = arrive(kc)
        for e in range(2):
            xe = xs[e * half:(e + 1) * half, :]
            for n0, n in chunks(ff, 256):
                acc_g[e, :, n0:n0 + n] += f32dot(xe, wg_buf[slot, e, :, n0:n0 + n])
                acc_u[e, :, n0:n0 + n] += f32dot(xe, wu_buf[slot, e, :, n0:n0 + n])

        @pl.when(kc + WRING < nk)
        def _():
            for c in w_copies(kc + WRING, slot):
                c.start()

        return carry

    lax.fori_loop(0, nk - 1, k_step, 0)

    slot = arrive(nk - 1)
    for e in range(2):
        xe = xs[e * half:(e + 1) * half, :]
        for n0, n in chunks(ff, 256):
            a = acc_g[e, :, n0:n0 + n] + f32dot(xe, wg_buf[slot, e, :, n0:n0 + n])
            b = acc_u[e, :, n0:n0 + n] + f32dot(xe, wu_buf[slot, e, :, n0:n0 + n])
            h[e, :, n0:n0 + n] = (a * (1.0 / (1.0 + jnp.exp(-a))) * b).astype(BF16)

    hc = CC // 2

    def a1_copy(s):
        return remote(o_a.at[s, :, 1], a1.at[s], a1_ss.at[s], a1_rs.at[s], 1)

    def a2_copy(s, k):
        return remote(a2s.at[s, k], a2.at[s, k], a2_ss.at[s, k], a2_rs.at[s, k], 2 * k)

    def b1_copy(s, k):
        return remote(o_b.at[s, pl.ds(k * ROWS, ROWS)], b1.at[s, k], b1_ss.at[s, k], b1_rs.at[s, k], 2 * k)

    def b2_copy(s):
        return remote(b2s.at[s], b2.at[s], b2_ss.at[s], b2_rs.at[s], 1)

    def stage1(s):
        slot = lax.rem(s, DRING)
        wd_copy(s, slot).wait()
        for e in range(2):
            parts[e * half:(e + 1) * half, :] = split3(f32dot(h[e], wd_buf[slot, e]))
        for k in range(4):
            at = slice(k * ROWS, (k + 1) * ROWS)
            g = gcol[at, :]
            v = sum3(f32dot(perm_t[at, :], parts[...]))
            va, vb = v[:, :hc] * g, v[:, hc:] * g
            o_a[s, k, 0] = va[:SLOTS]
            o_a[s, k, 1] = va[SLOTS:]
            if k == 0:
                b1[s, 0] = vb
            else:
                o_b[s, at] = vb
        a1_copy(s).start()
        for k in (2, 3, 1):
            b1_copy(s, k).start()

        @pl.when(s + DRING < ns)
        def _():
            wd_copy(s + DRING, slot).start()

    def stage2(s):
        a1_copy(s).wait_recv()
        for k in (2, 3, 1, 0):
            t = o_a[s, k, 0] + a1[s, k]
            if k == 0:
                a2[s, 0] = t
            else:
                a2s[s, k] = t
                a2_copy(s, k).start()
        for k in range(1, 4):
            b1_copy(s, k).wait_recv()
        blocks = b1[s]
        v = blocks[:, SLOTS:, :].reshape(4 * SLOTS, hc)
        b2s[s] = sum3(f32dot(merge[1], split3(v)))
        b2_copy(s).start()
        v = blocks[:, :SLOTS, :].reshape(4 * SLOTS, hc)
        own_b[s] = sum3(f32dot(merge[0], split3(v)))

    def stage3(s):
        for k in range(1, 4):
            a2_copy(s, k).wait_recv()
        v = a2[s].reshape(4 * SLOTS, hc)
        ya = sum3(f32dot(merge[0], split3(v)))
        b2_copy(s).wait_recv()
        yb = own_b[s] + b2[s]
        at = pl.ds(pl.multiple_of(s * CC, CC), CC)
        y_ref[:, at] = jnp.concatenate([ya, yb], axis=1).astype(BF16)

    def s_step(s, carry):
        @pl.when(s < ns)
        def _():
            stage1(s)

        @pl.when((s >= LAG1) & (s < ns + LAG1))
        def _():
            stage2(s - LAG1)

        @pl.when(s >= LAG2)
        def _():
            stage3(s - LAG2)

        return carry

    lax.fori_loop(0, ns + LAG2, s_step, 0)

    def d_done(kc, carry):
        for rel in range(1, 8):
            d_copy(kc, rel).wait_send()
        return carry

    lax.fori_loop(0, nk, d_done, 0)

    def s_done(s, carry):
        a1_copy(s).wait_send()
        b2_copy(s).wait_send()
        for k in range(1, 4):
            a2_copy(s, k).wait_send()
            b1_copy(s, k).wait_send()
        return carry

    lax.fori_loop(0, ns, s_done, 0)


def solution(mesh):
    row_spec = P(("dp", "ep", "tp"), None)

    def local_layer(tokens, expert_ids, gates, w_gate, w_up, w_down):
        rows, hidden = tokens.shape
        ff = w_gate.shape[2]
        nk, ns = hidden // KC, hidden // CC
        nq, hc = 8 * SLOTS, CC // 2
        meta = jnp.concatenate(
            [expert_ids.T.astype(F32), gates.T, jnp.zeros((4, rows), F32)], axis=0)
        vm, dma = pltpu.VMEM, pltpu.SemaphoreType.DMA
        scratch = [
            vm((8, 8, rows), F32),
            vm((nk, 4 * SLOTS, KC), BF16),
            vm((nk, nq, KC), BF16),
            vm((nq, KC), BF16),
            vm((WRING, 2, KC, ff), BF16),
            vm((WRING, 2, KC, ff), BF16),
            vm((DRING, 2, ff, CC), BF16),
            vm((2, nq // 2, ff), F32),
            vm((2, nq // 2, ff), F32),
            vm((2, nq // 2, ff), BF16),
            vm((nq, nq), BF16),
            vm((nq, nq), BF16),
            vm((2, rows, 4 * SLOTS), BF16),
            vm((nq, ROWS), F32),
            vm((nq, 3 * CC), BF16),
            vm((ns, 4, 2, SLOTS, hc), F32),
            vm((ns, nq, hc), F32),
            vm((ns, 4, SLOTS, hc), F32),
            vm((ns, 4, SLOTS, hc), F32),
            vm((ns, 4, SLOTS, hc), F32),
            vm((ns, 4, ROWS, hc), F32),
            vm((ns, ROWS, hc), F32),
            vm((ns, ROWS, hc), F32),
            vm((ns, ROWS, hc), F32),
            dma((8,)), dma((8,)), dma((nk, 8)), dma((nk, 8)), dma((2, WRING)), dma((DRING,)),
            dma((ns,)), dma((ns,)), dma((ns, 4)), dma((ns, 4)),
            dma((ns, 4)), dma((ns, 4)), dma((ns,)), dma((ns,)),
        ]
        vmem = pl.BlockSpec(memory_space=pltpu.VMEM)
        hbm = pl.BlockSpec(memory_space=pl.ANY)
        return pl.pallas_call(
            kernel,
            out_shape=jax.ShapeDtypeStruct((rows, hidden), BF16),
            in_specs=[vmem, vmem, hbm, hbm, hbm],
            out_specs=vmem,
            scratch_shapes=scratch,
            compiler_params=pltpu.CompilerParams(
                collective_id=0, has_side_effects=True, vmem_limit_bytes=67_000_000),
        )(meta, tokens, w_gate, w_up, w_down)

    return jax.shard_map(
        local_layer, mesh=mesh,
        in_specs=(row_spec, row_spec, row_spec, P("ep", None, "tp"), P("ep", None, "tp"), P("ep", "tp", None)),
        out_specs=row_spec, check_vma=False)
```

```python
import functools

import jax
import jax.numpy as jnp
from jax import lax
from jax.experimental import pallas as pl
from jax.experimental.pallas import tpu as pltpu
from jax.sharding import PartitionSpec as P

MESH = pl.DeviceIdType.MESH
F32 = jnp.float32
BF16 = jnp.bfloat16

ROWS = 128
SLOTS = 64
KC = 256
CC = 256
WRING = 3
MC = 1440
DRING = 2
LAG1, LAG2 = 1, 2


def f32dot(a, b):
    return jnp.dot(a, b, preferred_element_type=F32)


def ntdot(a, b):
    return lax.dot_general(a, b, (((1,), (1,)), ((), ())), preferred_element_type=F32)


def split3(v):
    hi = v.astype(BF16)
    rest = v - hi.astype(F32)
    mid = rest.astype(BF16)
    low = (rest - mid.astype(F32)).astype(BF16)
    return jnp.concatenate([hi, mid, low], axis=1)


def sum3(v):
    n = v.shape[1] // 3
    return (v[:, 2 * n:] + v[:, n:2 * n]) + v[:, :n]


def chunks(total, size):
    return [(i, min(size, total - i)) for i in range(0, total, size)]


def kernel(ids_ref, gates_ref, tok_ref, wg_hbm, wu_hbm, wd_hbm, y_ref,
           ids_all, gates_all, pack, slots, xs, wg_buf, wu_buf, wd_buf, acc_g, acc_u, h,
           perm, perm_t, merge, gcol, parts, o_a, o_b,
           a1, a2s, a2, b1, b2s, b2, own_b,
           id_ss, id_rs, gate_ss, gate_rs, d_ss, d_rs, w_sem, wd_sem,
           a1_ss, a1_rs, a2_ss, a2_rs, b1_ss, b1_rs, b2_ss, b2_rs):
    ep, tp = lax.axis_index("ep"), lax.axis_index("tp")
    core, x = lax.rem(ep, 2), lax.div(ep, 2)
    nk, ns = slots.shape[0], o_b.shape[0]
    ff = wg_buf.shape[2]

    def peer(rel):
        dx, dc, dy = rel // 4, (rel // 2) % 2, rel % 2
        return {"ep": lax.rem(x + dx, 2) * 2 + lax.rem(core + dc, 2), "tp": lax.rem(tp + dy, 2)}

    def ep_of(k):
        return lax.rem(x + k // 2, 2) * 2 + lax.rem(core + k % 2, 2)

    def w_copies(kc, slot):
        at = pl.ds(pl.multiple_of(kc * KC, KC), KC)
        return (pltpu.make_async_copy(wg_hbm.at[:, :, at], wg_buf.at[slot], w_sem.at[0, slot]),
                pltpu.make_async_copy(wu_hbm.at[:, :, at], wu_buf.at[slot], w_sem.at[1, slot]))

    def wd_copy(s, slot):
        at = pl.ds(pl.multiple_of(s * CC, CC), CC)
        return pltpu.make_async_copy(wd_hbm.at[:, :, at], wd_buf.at[slot], wd_sem.at[slot])

    def remote(src, dst, ss, rs, rel):
        return pltpu.make_async_remote_copy(src_ref=src, dst_ref=dst, send_sem=ss, recv_sem=rs,
                                            device_id=peer(rel), device_id_type=MESH)

    for i in range(WRING):
        for c in w_copies(i, i):
            c.start()
    for i in range(DRING):
        wd_copy(i, i).start()

    barrier = pltpu.get_barrier_semaphore()
    for rel in range(1, 8):
        pl.semaphore_signal(barrier, inc=1, device_id=peer(rel), device_id_type=MESH)
    pl.semaphore_wait(barrier, 7)

    def meta_copies(rel):
        return (remote(ids_ref, ids_all.at[rel], id_ss.at[rel], id_rs.at[rel], rel),
                remote(gates_ref, gates_all.at[rel], gate_ss.at[rel], gate_rs.at[rel], rel))

    for rel in range(1, 8):
        for c in meta_copies(rel):
            c.start()

    sub128 = lax.broadcasted_iota(jnp.int32, (ROWS, ROWS), 0)
    lane128 = lax.broadcasted_iota(jnp.int32, (ROWS, ROWS), 1)
    before = jnp.where(sub128 < lane128, 1.0, 0.0).astype(BF16)

    def select(ids, gates, epv):
        lo = 2.0 * epv.astype(F32)
        ids = ids.astype(F32)
        id0, id1, g0, g1 = ids[0:1, :], ids[1:2, :], gates[0:1, :], gates[1:2, :]
        first = (id0 >= lo) & (id0 <= lo + 1.0)
        second = (id1 >= lo) & (id1 <= lo + 1.0)
        mask = jnp.where(first | second, 1.0, 0.0)
        local = jnp.where(first, id0 - lo, jnp.where(second, id1 - lo, 0.0))
        gate = jnp.where(first, g0, jnp.where(second, g1, 0.0))
        return mask, local, gate

    def ranks(masks):
        m = jnp.concatenate(masks + masks[:1] * (8 - len(masks)), axis=0)
        r = f32dot(m.astype(BF16), before)
        return jnp.where(m > 0.5, r, -1.0)

    slot_iota = lax.broadcasted_iota(jnp.int32, (SLOTS, ROWS), 0).astype(F32)
    own = ranks([select(ids_ref[...], gates_ref[...], ep_of(k))[0] for k in range(4)])
    pick = jnp.concatenate(
        [jnp.where(own[k:k + 1, :] == slot_iota, 1.0, 0.0) for k in range(4)], axis=0).astype(BF16)

    def d_copy(kc, rel):
        k = rel // 2
        return remote(pack.at[kc, pl.ds(k * SLOTS, SLOTS)], slots.at[kc, pl.ds(rel * SLOTS, SLOTS)],
                      d_ss.at[kc, rel], d_rs.at[kc, rel], rel)

    for kc in range(nk):
        pack[kc] = f32dot(pick, tok_ref[:, kc * KC:(kc + 1) * KC]).astype(BF16)
        slots[kc, 0:SLOTS] = pack[kc, 0:SLOTS]
        for rel in (7, 4, 5, 6, 1, 3, 2):
            d_copy(kc, rel).start()

    acc_g[...] = jnp.zeros_like(acc_g)
    acc_u[...] = jnp.zeros_like(acc_u)

    for rel in range(1, 8):
        for c in meta_copies(rel):
            c.wait()
    ids_all[0] = ids_ref[...]
    gates_all[0] = gates_ref[...]

    chosen = [select(ids_all[rel], gates_all[rel], ep) for rel in range(8)]
    rank_in = ranks([c[0] for c in chosen])
    local_cols = []
    for rel in range(8):
        hit = rank_in[rel:rel + 1, :] == slot_iota
        local_cols.append(jnp.sum(jnp.where(hit, chosen[rel][1], 0.0), axis=1, keepdims=True))
        gcol[rel * SLOTS:(rel + 1) * SLOTS, :] = jnp.broadcast_to(
            jnp.sum(jnp.where(hit, chosen[rel][2], 0.0), axis=1, keepdims=True), (SLOTS, ROWS))
    nq = 8 * SLOTS
    local = jnp.concatenate([jnp.broadcast_to(c, (SLOTS, ROWS)) for c in local_cols], axis=0)
    q_sub = lax.broadcasted_iota(jnp.int32, (nq, nq), 0)
    q_lane = lax.broadcasted_iota(jnp.int32, (nq, nq), 1)
    after = jnp.where(q_sub > q_lane, 1.0, 0.0).astype(BF16)
    ones_before = f32dot(after, local.astype(BF16))
    q_col = lax.broadcasted_iota(jnp.int32, (nq, ROWS), 0).astype(F32)
    l_row = lax.broadcasted_iota(jnp.int32, (nq, ROWS), 1).astype(F32)
    place = jnp.where(local > 0.5, nq // 2 + ones_before, q_col - ones_before)
    diag = sub128 == lane128
    for j in range(nq // ROWS):
        at = slice(j * ROWS, (j + 1) * ROWS)
        perm_t[:, at] = jnp.where(place == l_row + float(j * ROWS), 1.0, 0.0).astype(BF16)
        row = jnp.sum(jnp.where(diag, place[at, :], 0.0), axis=0, keepdims=True)
        perm[:, at] = jnp.where(row == q_col, 1.0, 0.0).astype(BF16)

    s_lane = lane128.astype(F32)
    par = ranks([select(ids_all[1], gates_all[1], ep_of(k))[0] for k in range(4)])
    for who, r in enumerate((own, par)):
        cols = [jnp.sum(jnp.where(diag, r[k:k + 1, :], 0.0), axis=1, keepdims=True) for k in range(4)]
        for j in range(2):
            hit = jnp.where(s_lane < float(SLOTS), cols[2 * j] - s_lane,
                            cols[2 * j + 1] - s_lane + float(SLOTS)) == 0.0
            merge[who, :, j * ROWS:(j + 1) * ROWS] = jnp.where(hit, 1.0, 0.0).astype(BF16)

    half = nq // 2

    def arrive(kc):
        slot = lax.rem(kc, WRING)
        for rel in range(1, 8):
            d_copy(kc, rel).wait_recv()
        xs[...] = f32dot(perm[...], slots[kc]).astype(BF16)
        for c in w_copies(kc, slot):
            c.wait()
        return slot

    def k_step(kc, carry):
        slot = arrive(kc)
        for e in range(2):
            xe = xs[e * half:(e + 1) * half, :]
            for n0, n in chunks(ff, MC):
                at = slice(n0, n0 + n)
                acc_g[e, at, :] += ntdot(wg_buf[slot, e, at, :], xe)
                acc_u[e, at, :] += ntdot(wu_buf[slot, e, at, :], xe)

        @pl.when(kc + WRING < nk)
        def _():
            for c in w_copies(kc + WRING, slot):
                c.start()

        return carry

    lax.fori_loop(0, nk - 1, k_step, 0)

    slot = arrive(nk - 1)
    eye = jnp.where(lax.broadcasted_iota(jnp.int32, (half, half), 0)
                    == lax.broadcasted_iota(jnp.int32, (half, half), 1), 1.0, 0.0).astype(BF16)
    for e in range(2):
        xe = xs[e * half:(e + 1) * half, :]
        for n0, n in chunks(ff, 256):
            at = slice(n0, n0 + n)
            a = acc_g[e, at, :] + ntdot(wg_buf[slot, e, at, :], xe)
            b = acc_u[e, at, :] + ntdot(wu_buf[slot, e, at, :], xe)
            act = (a * (1.0 / (1.0 + jnp.exp(-a))) * b).astype(BF16)
            h[e, :, at] = ntdot(eye, act).astype(BF16)

    hc = CC // 2

    def a1_copy(s):
        return remote(o_a.at[s, :, 1], a1.at[s], a1_ss.at[s], a1_rs.at[s], 1)

    def a2_copy(s, k):
        return remote(a2s.at[s, k], a2.at[s, k], a2_ss.at[s, k], a2_rs.at[s, k], 2 * k)

    def b1_copy(s, k):
        return remote(o_b.at[s, pl.ds(k * ROWS, ROWS)], b1.at[s, k], b1_ss.at[s, k], b1_rs.at[s, k], 2 * k)

    def b2_copy(s):
        return remote(b2s.at[s], b2.at[s], b2_ss.at[s], b2_rs.at[s], 1)

    def stage1(s):
        slot = lax.rem(s, DRING)
        wd_copy(s, slot).wait()
        for e in range(2):
            parts[e * half:(e + 1) * half, :] = split3(f32dot(h[e], wd_buf[slot, e]))
        for k in range(4):
            at = slice(k * ROWS, (k + 1) * ROWS)
            g = gcol[at, :]
            v = sum3(f32dot(perm_t[at, :], parts[...]))
            va, vb = v[:, :hc] * g, v[:, hc:] * g
            o_a[s, k, 0] = va[:SLOTS]
            o_a[s, k, 1] = va[SLOTS:]
            if k == 0:
                b1[s, 0] = vb
            else:
                o_b[s, at] = vb
        a1_copy(s).start()
        for k in (2, 3, 1):
            b1_copy(s, k).start()

        @pl.when(s + DRING < ns)
        def _():
            wd_copy(s + DRING, slot).start()

    def stage2(s):
        a1_copy(s).wait_recv()
        for k in (2, 3, 1, 0):
            t = o_a[s, k, 0] + a1[s, k]
            if k == 0:
                a2[s, 0] = t
            else:
                a2s[s, k] = t
                a2_copy(s, k).start()
        for k in range(1, 4):
            b1_copy(s, k).wait_recv()
        blocks = b1[s]
        v = blocks[:, SLOTS:, :].reshape(4 * SLOTS, hc)
        b2s[s] = sum3(f32dot(merge[1], split3(v)))
        b2_copy(s).start()
        v = blocks[:, :SLOTS, :].reshape(4 * SLOTS, hc)
        own_b[s] = sum3(f32dot(merge[0], split3(v)))

    def stage3(s):
        for k in range(1, 4):
            a2_copy(s, k).wait_recv()
        v = a2[s].reshape(4 * SLOTS, hc)
        ya = sum3(f32dot(merge[0], split3(v)))
        b2_copy(s).wait_recv()
        yb = own_b[s] + b2[s]
        at = pl.ds(pl.multiple_of(s * CC, CC), CC)
        y_ref[:, at] = jnp.concatenate([ya, yb], axis=1).astype(BF16)

    def s_step(s, carry):
        @pl.when(s < ns)
        def _():
            stage1(s)

        @pl.when((s >= LAG1) & (s < ns + LAG1))
        def _():
            stage2(s - LAG1)

        @pl.when(s >= LAG2)
        def _():
            stage3(s - LAG2)

        return carry

    lax.fori_loop(0, ns + LAG2, s_step, 0)

    def d_done(kc, carry):
        for rel in range(1, 8):
            d_copy(kc, rel).wait_send()
        return carry

    lax.fori_loop(0, nk, d_done, 0)

    def s_done(s, carry):
        a1_copy(s).wait_send()
        b2_copy(s).wait_send()
        for k in range(1, 4):
            a2_copy(s, k).wait_send()
            b1_copy(s, k).wait_send()
        return carry

    lax.fori_loop(0, ns, s_done, 0)


def solution(mesh):
    row_spec = P(("dp", "ep", "tp"), None)

    def local_layer(tokens, expert_ids, gates, w_gate, w_up, w_down):
        rows, hidden = tokens.shape
        ff = w_gate.shape[2]
        nk, ns = hidden // KC, hidden // CC
        nq, hc = 8 * SLOTS, CC // 2
        vm, dma = pltpu.VMEM, pltpu.SemaphoreType.DMA
        scratch = [
            vm((8, 2, rows), jnp.int32),
            vm((8, 2, rows), F32),
            vm((nk, 4 * SLOTS, KC), BF16),
            vm((nk, nq, KC), BF16),
            vm((nq, KC), BF16),
            vm((WRING, 2, ff, KC), BF16),
            vm((WRING, 2, ff, KC), BF16),
            vm((DRING, 2, ff, CC), BF16),
            vm((2, ff, nq // 2), F32),
            vm((2, ff, nq // 2), F32),
            vm((2, nq // 2, ff), BF16),
            vm((nq, nq), BF16),
            vm((nq, nq), BF16),
            vm((2, rows, 4 * SLOTS), BF16),
            vm((nq, ROWS), F32),
            vm((nq, 3 * CC), BF16),
            vm((ns, 4, 2, SLOTS, hc), F32),
            vm((ns, nq, hc), F32),
            vm((ns, 4, SLOTS, hc), F32),
            vm((ns, 4, SLOTS, hc), F32),
            vm((ns, 4, SLOTS, hc), F32),
            vm((ns, 4, ROWS, hc), F32),
            vm((ns, ROWS, hc), F32),
            vm((ns, ROWS, hc), F32),
            vm((ns, ROWS, hc), F32),
            dma((8,)), dma((8,)), dma((8,)), dma((8,)), dma((nk, 8)), dma((nk, 8)), dma((2, WRING)), dma((DRING,)),
            dma((ns,)), dma((ns,)), dma((ns, 4)), dma((ns, 4)),
            dma((ns, 4)), dma((ns, 4)), dma((ns,)), dma((ns,)),
        ]
        vmem = pl.BlockSpec(memory_space=pltpu.VMEM)
        hbm = pl.BlockSpec(memory_space=pl.ANY)
        return pl.pallas_call(
            kernel,
            out_shape=jax.ShapeDtypeStruct((rows, hidden), BF16),
            in_specs=[vmem, vmem, vmem, hbm, hbm, hbm],
            out_specs=vmem,
            scratch_shapes=scratch,
            compiler_params=pltpu.CompilerParams(
                collective_id=0, has_side_effects=True, vmem_limit_bytes=67_000_000),
        )(expert_ids.T, gates.T, tokens, w_gate.swapaxes(1, 2), w_up.swapaxes(1, 2), w_down)

    return jax.shard_map(
        local_layer, mesh=mesh,
        in_specs=(row_spec, row_spec, row_spec, P("ep", None, "tp"), P("ep", None, "tp"), P("ep", "tp", None)),
        out_specs=row_spec, check_vma=False)
```

```python
import functools

import jax
import jax.numpy as jnp
from jax import lax
from jax.experimental import pallas as pl
from jax.experimental.pallas import tpu as pltpu
from jax.sharding import PartitionSpec as P

MESH = pl.DeviceIdType.MESH
F32 = jnp.float32
BF16 = jnp.bfloat16

ROWS = 128
SLOTS = 64
KC = 256
CC = 256
WRING = 3
WFIRST = 1
MC = 1440
DRING = 2
LAG1, LAG2 = 1, 2


def f32dot(a, b):
    return jnp.dot(a, b, preferred_element_type=F32)


def ntdot(a, b):
    return lax.dot_general(a, b, (((1,), (1,)), ((), ())), preferred_element_type=F32)


def split3(v):
    hi = v.astype(BF16)
    rest = v - hi.astype(F32)
    mid = rest.astype(BF16)
    low = (rest - mid.astype(F32)).astype(BF16)
    return jnp.concatenate([hi, mid, low], axis=1)


def sum3(v):
    n = v.shape[1] // 3
    return (v[:, 2 * n:] + v[:, n:2 * n]) + v[:, :n]


def chunks(total, size):
    return [(i, min(size, total - i)) for i in range(0, total, size)]


def kernel(ids_ref, gates_ref, tok_ref, wg_hbm, wu_hbm, wd_hbm, y_ref,
           ids_all, gates_all, pack, dense, repack, slots, xs, wg_buf, wu_buf, wd_buf, acc_g, acc_u, h,
           pick_par, perm, perm_t, merge, gcol, parts, o_a, o_b,
           a1, a2s, a2, b1, b2s, b2, own_b,
           id_ss, id_rs, gate_ss, gate_rs, d_ss, d_rs, w_sem, wd_sem,
           a1_ss, a1_rs, a2_ss, a2_rs, b1_ss, b1_rs, b2_ss, b2_rs):
    ep, tp = lax.axis_index("ep"), lax.axis_index("tp")
    core, x = lax.rem(ep, 2), lax.div(ep, 2)
    nk, ns = slots.shape[0], o_b.shape[0]
    ff = wg_buf.shape[2]

    def peer(rel):
        dx, dc, dy = rel // 4, (rel // 2) % 2, rel % 2
        return {"ep": lax.rem(x + dx, 2) * 2 + lax.rem(core + dc, 2), "tp": lax.rem(tp + dy, 2)}

    def ep_of(k):
        return lax.rem(x + k // 2, 2) * 2 + lax.rem(core + k % 2, 2)

    def w_copies(kc, slot):
        at = pl.ds(pl.multiple_of(kc * KC, KC), KC)
        return (pltpu.make_async_copy(wg_hbm.at[:, :, at], wg_buf.at[slot], w_sem.at[0, slot]),
                pltpu.make_async_copy(wu_hbm.at[:, :, at], wu_buf.at[slot], w_sem.at[1, slot]))

    def wd_copy(s, slot):
        at = pl.ds(pl.multiple_of(s * CC, CC), CC)
        return pltpu.make_async_copy(wd_hbm.at[:, :, at], wd_buf.at[slot], wd_sem.at[slot])

    def remote(src, dst, ss, rs, rel):
        return pltpu.make_async_remote_copy(src_ref=src, dst_ref=dst, send_sem=ss, recv_sem=rs,
                                            device_id=peer(rel), device_id_type=MESH)

    barrier = pltpu.get_barrier_semaphore()
    for rel in range(1, 8):
        pl.semaphore_signal(barrier, inc=1, device_id=peer(rel), device_id_type=MESH)
    for i in range(WFIRST):
        for c in w_copies(i, i):
            c.start()

    def meta_copies(rel):
        return (remote(ids_ref, ids_all.at[rel], id_ss.at[rel], id_rs.at[rel], rel),
                remote(gates_ref, gates_all.at[rel], gate_ss.at[rel], gate_rs.at[rel], rel))


    sub128 = lax.broadcasted_iota(jnp.int32, (ROWS, ROWS), 0)
    lane128 = lax.broadcasted_iota(jnp.int32, (ROWS, ROWS), 1)
    before = jnp.where(sub128 < lane128, 1.0, 0.0).astype(BF16)

    def select(ids, gates, epv):
        lo = 2.0 * epv.astype(F32)
        ids = ids.astype(F32)
        id0, id1, g0, g1 = ids[0:1, :], ids[1:2, :], gates[0:1, :], gates[1:2, :]
        first = (id0 >= lo) & (id0 <= lo + 1.0)
        second = (id1 >= lo) & (id1 <= lo + 1.0)
        mask = jnp.where(first | second, 1.0, 0.0)
        local = jnp.where(first, id0 - lo, jnp.where(second, id1 - lo, 0.0))
        gate = jnp.where(first, g0, jnp.where(second, g1, 0.0))
        return mask, local, gate

    def ranks(masks):
        m = jnp.concatenate(masks + masks[:1] * (8 - len(masks)), axis=0)
        r = f32dot(m.astype(BF16), before)
        return jnp.where(m > 0.5, r, -1.0)

    slot_iota = lax.broadcasted_iota(jnp.int32, (SLOTS, ROWS), 0).astype(F32)
    own = ranks([select(ids_ref[...], gates_ref[...], ep_of(k))[0] for k in range(4)])

    def picks(r):
        return jnp.concatenate(
            [jnp.where(r[k:k + 1, :] == slot_iota, 1.0, 0.0) for k in range(4)], axis=0).astype(BF16)

    pick = picks(own)

    def d_copy(kc, block, src, to):
        return remote(src, slots.at[kc, pl.ds(block * SLOTS, SLOTS)],
                      d_ss.at[kc, block], d_rs.at[kc, block], to)

    def packed(kc, rel):
        return d_copy(kc, rel, pack.at[kc, pl.ds(rel // 2 * SLOTS, SLOTS)], rel)

    def handed(kc, block):
        return d_copy(kc, block, slots.at[kc, pl.ds((block - 1) * SLOTS, SLOTS)], 1)

    def repacked(kc, block):
        return d_copy(kc, block, repack.at[lax.div(kc, 2), pl.ds(block // 2 * SLOTS, SLOTS)], block - 1)

    def dense_copy(kc):
        at = pl.ds(pl.multiple_of(kc * KC, KC), KC)
        return remote(tok_ref.at[:, at], dense.at[lax.div(kc, 2)], d_ss.at[kc, 1], d_rs.at[kc, 1], 1)

    def send(kc, way):
        if way == "y":
            dense_copy(kc).start()
        for rel in {"x": (4, 6, 1, 3, 2), "y": (4, 6, 2), "direct": (7, 5, 4, 6, 1, 3, 2)}[way]:
            packed(kc, rel).start()

    def relay(kc, way):
        if way == "x":
            for block in (5, 7):
                packed(kc, block - 1).wait_recv()
                handed(kc, block).start()
        else:
            dense_copy(kc).wait_recv()
            j = lax.div(kc, 2)
            repack[j] = f32dot(pick_par[...], dense[j]).astype(BF16)
            slots[kc, SLOTS:2 * SLOTS] = repack[j, 0:SLOTS]
            for block in (5, 7, 3):
                repacked(kc, block).start()

    def take(kc, way):
        for block in {"x": (1, 2, 3, 5, 7), "y": (2, 3, 4, 5, 6, 7), "direct": range(1, 8)}[way]:
            packed(kc, block).wait_recv()

    def sent(kc, way):
        if way == "y":
            dense_copy(kc).wait_send()
        for block in range(2 if way == "y" else 1, 8):
            packed(kc, block).wait_send()

    def by_way(kc, act):
        @pl.when(lax.rem(kc, 2) == 0)
        def _():
            act(kc, "x")

        @pl.when(lax.rem(kc, 2) == 1)
        def _():
            act(kc, "y")

    for kc in range(nk):
        pack[kc] = f32dot(pick, tok_ref[:, kc * KC:(kc + 1) * KC]).astype(BF16)
        slots[kc, 0:SLOTS] = pack[kc, 0:SLOTS]
    pl.semaphore_wait(barrier, 7)
    for rel in range(1, 8):
        for c in meta_copies(rel):
            c.start()
    for kc in range(3):
        send(kc, "xy"[kc % 2])
    for i in range(WFIRST, WRING):
        for c in w_copies(i, i):
            c.start()
    for i in range(DRING):
        wd_copy(i, i).start()

    acc_g[...] = jnp.zeros_like(acc_g)
    acc_u[...] = jnp.zeros_like(acc_u)

    for rel in range(1, 8):
        for c in meta_copies(rel):
            c.wait()
    ids_all[0] = ids_ref[...]
    gates_all[0] = gates_ref[...]

    chosen = [select(ids_all[rel], gates_all[rel], ep) for rel in range(8)]
    rank_in = ranks([c[0] for c in chosen])
    local_cols = []
    for rel in range(8):
        hit = rank_in[rel:rel + 1, :] == slot_iota
        local_cols.append(jnp.sum(jnp.where(hit, chosen[rel][1], 0.0), axis=1, keepdims=True))
        gcol[rel * SLOTS:(rel + 1) * SLOTS, :] = jnp.broadcast_to(
            jnp.sum(jnp.where(hit, chosen[rel][2], 0.0), axis=1, keepdims=True), (SLOTS, ROWS))
    nq = 8 * SLOTS
    local = jnp.concatenate([jnp.broadcast_to(c, (SLOTS, ROWS)) for c in local_cols], axis=0)
    q_sub = lax.broadcasted_iota(jnp.int32, (nq, nq), 0)
    q_lane = lax.broadcasted_iota(jnp.int32, (nq, nq), 1)
    after = jnp.where(q_sub > q_lane, 1.0, 0.0).astype(BF16)
    ones_before = f32dot(after, local.astype(BF16))
    q_col = lax.broadcasted_iota(jnp.int32, (nq, ROWS), 0).astype(F32)
    l_row = lax.broadcasted_iota(jnp.int32, (nq, ROWS), 1).astype(F32)
    place = jnp.where(local > 0.5, nq // 2 + ones_before, q_col - ones_before)
    diag = sub128 == lane128
    for j in range(nq // ROWS):
        at = slice(j * ROWS, (j + 1) * ROWS)
        perm_t[:, at] = jnp.where(place == l_row + float(j * ROWS), 1.0, 0.0).astype(BF16)
        row = jnp.sum(jnp.where(diag, place[at, :], 0.0), axis=0, keepdims=True)
        perm[:, at] = jnp.where(row == q_col, 1.0, 0.0).astype(BF16)

    s_lane = lane128.astype(F32)
    par = ranks([select(ids_all[1], gates_all[1], ep_of(k))[0] for k in range(4)])
    pick_par[...] = picks(par)
    for who, r in enumerate((own, par)):
        cols = [jnp.sum(jnp.where(diag, r[k:k + 1, :], 0.0), axis=1, keepdims=True) for k in range(4)]
        for j in range(2):
            hit = jnp.where(s_lane < float(SLOTS), cols[2 * j] - s_lane,
                            cols[2 * j + 1] - s_lane + float(SLOTS)) == 0.0
            merge[who, :, j * ROWS:(j + 1) * ROWS] = jnp.where(hit, 1.0, 0.0).astype(BF16)

    half = nq // 2

    def arrive(kc):
        slot = lax.rem(kc, WRING)
        xs[...] = f32dot(perm[...], slots[kc]).astype(BF16)
        for c in w_copies(kc, slot):
            c.wait()
        return slot

    last = nk - 1
    for kc in range(3):
        relay(kc, "xy"[kc % 2])
        send(kc + 3, "xy"[(kc + 3) % 2])

    def k_step(kc, carry):
        @pl.when((kc >= 1) & (kc + 2 < last))
        def _():
            by_way(kc + 2, relay)

        @pl.when((kc >= 1) & (kc + 5 < last))
        def _():
            by_way(kc + 5, send)

        @pl.when(kc + 3 == last)
        def _():
            send(last, "direct")

        by_way(kc, take)
        slot = arrive(kc)
        for e in range(2):
            xe = xs[e * half:(e + 1) * half, :]
            for n0, n in chunks(ff, MC):
                at = slice(n0, n0 + n)
                acc_g[e, at, :] += ntdot(wg_buf[slot, e, at, :], xe)
                acc_u[e, at, :] += ntdot(wu_buf[slot, e, at, :], xe)

        @pl.when(kc + WRING < nk)
        def _():
            for c in w_copies(kc + WRING, slot):
                c.start()

        return carry

    lax.fori_loop(0, nk - 1, k_step, 0)

    take(last, "direct")
    slot = arrive(last)
    for e in range(2):
        xe = xs[e * half:(e + 1) * half, :]
        for n0, n in chunks(ff, 256):
            at = slice(n0, n0 + n)
            a = acc_g[e, at, :] + ntdot(wg_buf[slot, e, at, :], xe)
            b = acc_u[e, at, :] + ntdot(wu_buf[slot, e, at, :], xe)
            act = (a * (1.0 / (1.0 + jnp.exp(-a))) * b).astype(BF16)
            h[e, :, at] = act.T

    hc = CC // 2

    def a1_copy(s):
        return remote(o_a.at[s, :, 1], a1.at[s], a1_ss.at[s], a1_rs.at[s], 1)

    def a2_copy(s, k):
        return remote(a2s.at[s, k], a2.at[s, k], a2_ss.at[s, k], a2_rs.at[s, k], 2 * k)

    def b1_copy(s, k):
        return remote(o_b.at[s, pl.ds(k * ROWS, ROWS)], b1.at[s, k], b1_ss.at[s, k], b1_rs.at[s, k], 2 * k)

    def b2_copy(s):
        return remote(b2s.at[s], b2.at[s], b2_ss.at[s], b2_rs.at[s], 1)

    def stage1(s):
        slot = lax.rem(s, DRING)
        wd_copy(s, slot).wait()
        for e in range(2):
            parts[e * half:(e + 1) * half, :] = split3(f32dot(h[e], wd_buf[slot, e]))
        for k in range(4):
            at = slice(k * ROWS, (k + 1) * ROWS)
            g = gcol[at, :]
            v = sum3(f32dot(perm_t[at, :], parts[...]))
            va, vb = v[:, :hc] * g, v[:, hc:] * g
            o_a[s, k, 0] = va[:SLOTS]
            o_a[s, k, 1] = va[SLOTS:]
            if k == 0:
                b1[s, 0] = vb
            else:
                o_b[s, at] = vb
        a1_copy(s).start()
        for k in (2, 3, 1):
            b1_copy(s, k).start()

        @pl.when(s + DRING < ns)
        def _():
            wd_copy(s + DRING, slot).start()

    def stage2(s):
        a1_copy(s).wait_recv()
        for k in (2, 3, 1, 0):
            t = o_a[s, k, 0] + a1[s, k]
            if k == 0:
                a2[s, 0] = t
            else:
                a2s[s, k] = t
                a2_copy(s, k).start()
        for k in range(1, 4):
            b1_copy(s, k).wait_recv()
        blocks = b1[s]
        v = blocks[:, SLOTS:, :].reshape(4 * SLOTS, hc)
        b2s[s] = sum3(f32dot(merge[1], split3(v)))
        b2_copy(s).start()
        v = blocks[:, :SLOTS, :].reshape(4 * SLOTS, hc)
        own_b[s] = sum3(f32dot(merge[0], split3(v)))

    def stage3(s):
        for k in range(1, 4):
            a2_copy(s, k).wait_recv()
        v = a2[s].reshape(4 * SLOTS, hc)
        ya = sum3(f32dot(merge[0], split3(v)))
        b2_copy(s).wait_recv()
        yb = own_b[s] + b2[s]
        at = pl.ds(pl.multiple_of(s * CC, CC), CC)
        y_ref[:, at] = jnp.concatenate([ya, yb], axis=1).astype(BF16)

    def s_step(s, carry):
        @pl.when(s < ns)
        def _():
            stage1(s)

        @pl.when((s >= LAG1) & (s < ns + LAG1))
        def _():
            stage2(s - LAG1)

        @pl.when(s >= LAG2)
        def _():
            stage3(s - LAG2)

        return carry

    lax.fori_loop(0, ns + LAG2, s_step, 0)

    def d_done(kc, carry):
        by_way(kc, sent)
        return carry

    lax.fori_loop(0, last, d_done, 0)
    sent(last, "direct")

    def s_done(s, carry):
        a1_copy(s).wait_send()
        b2_copy(s).wait_send()
        for k in range(1, 4):
            a2_copy(s, k).wait_send()
            b1_copy(s, k).wait_send()
        return carry

    lax.fori_loop(0, ns, s_done, 0)


def solution(mesh):
    row_spec = P(("dp", "ep", "tp"), None)

    def local_layer(tokens, expert_ids, gates, w_gate, w_up, w_down):
        rows, hidden = tokens.shape
        ff = w_gate.shape[2]
        nk, ns = hidden // KC, hidden // CC
        nq, hc = 8 * SLOTS, CC // 2
        vm, dma = pltpu.VMEM, pltpu.SemaphoreType.DMA
        scratch = [
            vm((8, 2, rows), jnp.int32),
            vm((8, 2, rows), F32),
            vm((nk, 4 * SLOTS, KC), BF16),
            vm((nk // 2, rows, KC), BF16),
            vm((nk // 2, 4 * SLOTS, KC), BF16),
            vm((nk, nq, KC), BF16),
            vm((nq, KC), BF16),
            vm((WRING, 2, ff, KC), BF16),
            vm((WRING, 2, ff, KC), BF16),
            vm((DRING, 2, ff, CC), BF16),
            vm((2, ff, nq // 2), F32),
            vm((2, ff, nq // 2), F32),
            vm((2, nq // 2, ff), BF16),
            vm((4 * SLOTS, rows), BF16),
            vm((nq, nq), BF16),
            vm((nq, nq), BF16),
            vm((2, rows, 4 * SLOTS), BF16),
            vm((nq, ROWS), F32),
            vm((nq, 3 * CC), BF16),
            vm((ns, 4, 2, SLOTS, hc), F32),
            vm((ns, nq, hc), F32),
            vm((ns, 4, SLOTS, hc), F32),
            vm((ns, 4, SLOTS, hc), F32),
            vm((ns, 4, SLOTS, hc), F32),
            vm((ns, 4, ROWS, hc), F32),
            vm((ns, ROWS, hc), F32),
            vm((ns, ROWS, hc), F32),
            vm((ns, ROWS, hc), F32),
            dma((8,)), dma((8,)), dma((8,)), dma((8,)), dma((nk, 8)), dma((nk, 8)), dma((2, WRING)), dma((DRING,)),
            dma((ns,)), dma((ns,)), dma((ns, 4)), dma((ns, 4)),
            dma((ns, 4)), dma((ns, 4)), dma((ns,)), dma((ns,)),
        ]
        vmem = pl.BlockSpec(memory_space=pltpu.VMEM)
        hbm = pl.BlockSpec(memory_space=pl.ANY)
        return pl.pallas_call(
            kernel,
            out_shape=jax.ShapeDtypeStruct((rows, hidden), BF16),
            in_specs=[vmem, vmem, vmem, hbm, hbm, hbm],
            out_specs=vmem,
            scratch_shapes=scratch,
            compiler_params=pltpu.CompilerParams(
                collective_id=0, has_side_effects=True, vmem_limit_bytes=67_000_000),
        )(expert_ids.T, gates.T, tokens, w_gate.swapaxes(1, 2), w_up.swapaxes(1, 2), w_down)

    return jax.shard_map(
        local_layer, mesh=mesh,
        in_specs=(row_spec, row_spec, row_spec, P("ep", None, "tp"), P("ep", None, "tp"), P("ep", "tp", None)),
        out_specs=row_spec, check_vma=False)
```

```python
import functools

import jax
import jax.numpy as jnp
from jax import lax
from jax.experimental import pallas as pl
from jax.experimental.pallas import tpu as pltpu
from jax.sharding import PartitionSpec as P

MESH = pl.DeviceIdType.MESH
F32 = jnp.float32
BF16 = jnp.bfloat16

ROWS = 128
SLOTS = 64
KC = 256
CC = 256
WRING = 3
WFIRST = 1
MC = 1440
DRING = 2
LAG1, LAG2 = 3, 6
AHEAD = 3
RELAYS = 3
RELAYED = 8


def f32dot(a, b):
    return jnp.dot(a, b, preferred_element_type=F32)


def ntdot(a, b):
    return lax.dot_general(a, b, (((1,), (1,)), ((), ())), preferred_element_type=F32)


def split3(v):
    hi = v.astype(BF16)
    rest = v - hi.astype(F32)
    mid = rest.astype(BF16)
    low = (rest - mid.astype(F32)).astype(BF16)
    return jnp.concatenate([hi, mid, low], axis=1)


def sum3(v):
    n = v.shape[1] // 3
    return (v[:, 2 * n:] + v[:, n:2 * n]) + v[:, :n]


def chunks(total, size):
    return [(i, min(size, total - i)) for i in range(0, total, size)]


def kernel(ids_ref, gates_ref, tok_ref, wg_hbm, wu_hbm, wd_hbm, y_ref,
           ids_all, gates_all, pack, dense, repack, slots, xs, wg_buf, wu_buf, wd_buf, acc_g, acc_u, h,
           pick_par, perm, perm_t, merge, gcol, parts, o_a, o_b,
           a1, a2s, a2, b1, b2s, b2, own_b,
           id_ss, id_rs, gate_ss, gate_rs, d_ss, d_rs, w_sem, wd_sem,
           a1_ss, a1_rs, a2_ss, a2_rs, b1_ss, b1_rs, b2_ss, b2_rs):
    ep, tp = lax.axis_index("ep"), lax.axis_index("tp")
    core, x = lax.rem(ep, 2), lax.div(ep, 2)
    nk, ns = slots.shape[0], o_b.shape[0]
    ff = wg_buf.shape[2]

    def peer(rel):
        dx, dc, dy = rel // 4, (rel // 2) % 2, rel % 2
        return {"ep": lax.rem(x + dx, 2) * 2 + lax.rem(core + dc, 2), "tp": lax.rem(tp + dy, 2)}

    def ep_of(k):
        return lax.rem(x + k // 2, 2) * 2 + lax.rem(core + k % 2, 2)

    def w_copies(kc, slot):
        at = pl.ds(pl.multiple_of(kc * KC, KC), KC)
        return (pltpu.make_async_copy(wg_hbm.at[:, :, at], wg_buf.at[slot], w_sem.at[0, slot]),
                pltpu.make_async_copy(wu_hbm.at[:, :, at], wu_buf.at[slot], w_sem.at[1, slot]))

    def wd_copy(s, slot):
        at = pl.ds(pl.multiple_of(s * CC, CC), CC)
        return pltpu.make_async_copy(wd_hbm.at[:, :, at], wd_buf.at[slot], wd_sem.at[slot])

    def remote(src, dst, ss, rs, rel):
        return pltpu.make_async_remote_copy(src_ref=src, dst_ref=dst, send_sem=ss, recv_sem=rs,
                                            device_id=peer(rel), device_id_type=MESH)

    barrier = pltpu.get_barrier_semaphore()
    for rel in range(1, 8):
        pl.semaphore_signal(barrier, inc=1, device_id=peer(rel), device_id_type=MESH)
    for i in range(WFIRST):
        for c in w_copies(i, i):
            c.start()

    def meta_copies(rel):
        return (remote(ids_ref, ids_all.at[rel], id_ss.at[rel], id_rs.at[rel], rel),
                remote(gates_ref, gates_all.at[rel], gate_ss.at[rel], gate_rs.at[rel], rel))


    sub128 = lax.broadcasted_iota(jnp.int32, (ROWS, ROWS), 0)
    lane128 = lax.broadcasted_iota(jnp.int32, (ROWS, ROWS), 1)
    before = jnp.where(sub128 < lane128, 1.0, 0.0).astype(BF16)

    def select(ids, gates, epv):
        lo = 2.0 * epv.astype(F32)
        ids = ids.astype(F32)
        id0, id1, g0, g1 = ids[0:1, :], ids[1:2, :], gates[0:1, :], gates[1:2, :]
        first = (id0 >= lo) & (id0 <= lo + 1.0)
        second = (id1 >= lo) & (id1 <= lo + 1.0)
        mask = jnp.where(first | second, 1.0, 0.0)
        local = jnp.where(first, id0 - lo, jnp.where(second, id1 - lo, 0.0))
        gate = jnp.where(first, g0, jnp.where(second, g1, 0.0))
        return mask, local, gate

    def ranks(masks):
        m = jnp.concatenate(masks + masks[:1] * (8 - len(masks)), axis=0)
        r = f32dot(m.astype(BF16), before)
        return jnp.where(m > 0.5, r, -1.0)

    slot_iota = lax.broadcasted_iota(jnp.int32, (SLOTS, ROWS), 0).astype(F32)
    own = ranks([select(ids_ref[...], gates_ref[...], ep_of(k))[0] for k in range(4)])

    def picks(r):
        return jnp.concatenate(
            [jnp.where(r[k:k + 1, :] == slot_iota, 1.0, 0.0) for k in range(4)], axis=0).astype(BF16)

    pick = picks(own)

    def d_copy(kc, block, src, to):
        return remote(src, slots.at[kc, pl.ds(block * SLOTS, SLOTS)],
                      d_ss.at[kc, block], d_rs.at[kc, block], to)

    def packed(kc, rel):
        return d_copy(kc, rel, pack.at[kc, pl.ds(rel // 2 * SLOTS, SLOTS)], rel)

    def handed(kc, block):
        return d_copy(kc, block, slots.at[kc, pl.ds((block - 1) * SLOTS, SLOTS)], 1)

    def repacked(kc, block):
        return d_copy(kc, block, repack.at[lax.div(kc, 2), pl.ds(block // 2 * SLOTS, SLOTS)], block - 1)

    def dense_copy(kc):
        at = pl.ds(pl.multiple_of(kc * KC, KC), KC)
        return remote(tok_ref.at[:, at], dense.at[lax.div(kc, 2)], d_ss.at[kc, 1], d_rs.at[kc, 1], 1)

    def send(kc, way):
        if way == "y":
            dense_copy(kc).start()
        for rel in {"x": (4, 6, 1, 3, 2), "y": (4, 6, 2), "direct": (7, 5, 4, 6, 1, 3, 2)}[way]:
            packed(kc, rel).start()

    def relay(kc, way):
        if way == "x":
            for block in (5, 7):
                packed(kc, block - 1).wait_recv()
                handed(kc, block).start()
        if way == "y":
            dense_copy(kc).wait_recv()
            j = lax.div(kc, 2)
            repack[j] = f32dot(pick_par[...], dense[j]).astype(BF16)
            slots[kc, SLOTS:2 * SLOTS] = repack[j, 0:SLOTS]
            for block in (5, 7, 3):
                repacked(kc, block).start()

    def take(kc, way):
        for block in {"x": (1, 2, 3, 5, 7), "y": (2, 3, 4, 5, 6, 7), "direct": range(1, 8)}[way]:
            packed(kc, block).wait_recv()

    def sent(kc, way):
        if way == "y":
            dense_copy(kc).wait_send()
        for block in range(2 if way == "y" else 1, 8):
            packed(kc, block).wait_send()

    last = nk - 1

    def way_of(kc):
        return "xy"[kc % 2] if kc < RELAYED else "direct"

    def by_way(kc, act, ok=True):
        if isinstance(kc, int):
            act(kc, way_of(kc))
            return
        for i, way in enumerate(("x", "y")):
            @pl.when((lax.rem(kc, 2) == i) & (kc < RELAYED) & ok)
            def _():
                act(kc, way)

        @pl.when((kc >= RELAYED) & ok)
        def _():
            act(kc, "direct")

    for kc in range(nk):
        pack[kc] = f32dot(pick, tok_ref[:, kc * KC:(kc + 1) * KC]).astype(BF16)
        slots[kc, 0:SLOTS] = pack[kc, 0:SLOTS]
    pl.semaphore_wait(barrier, 7)
    for rel in range(1, 8):
        for c in meta_copies(rel):
            c.start()
    for kc in range(AHEAD):
        by_way(kc, send)
    for i in range(WFIRST, WRING):
        for c in w_copies(i, i):
            c.start()
    for i in range(DRING):
        wd_copy(i, i).start()

    acc_g[...] = jnp.zeros_like(acc_g)
    acc_u[...] = jnp.zeros_like(acc_u)

    for rel in range(1, 8):
        for c in meta_copies(rel):
            c.wait()
    ids_all[0] = ids_ref[...]
    gates_all[0] = gates_ref[...]

    chosen = [select(ids_all[rel], gates_all[rel], ep) for rel in range(8)]
    rank_in = ranks([c[0] for c in chosen])
    local_cols = []
    for rel in range(8):
        hit = rank_in[rel:rel + 1, :] == slot_iota
        local_cols.append(jnp.sum(jnp.where(hit, chosen[rel][1], 0.0), axis=1, keepdims=True))
        gcol[rel * SLOTS:(rel + 1) * SLOTS, :] = jnp.broadcast_to(
            jnp.sum(jnp.where(hit, chosen[rel][2], 0.0), axis=1, keepdims=True), (SLOTS, ROWS))
    nq = 8 * SLOTS
    local = jnp.concatenate([jnp.broadcast_to(c, (SLOTS, ROWS)) for c in local_cols], axis=0)
    q_sub = lax.broadcasted_iota(jnp.int32, (nq, nq), 0)
    q_lane = lax.broadcasted_iota(jnp.int32, (nq, nq), 1)
    after = jnp.where(q_sub > q_lane, 1.0, 0.0).astype(BF16)
    ones_before = f32dot(after, local.astype(BF16))
    q_col = lax.broadcasted_iota(jnp.int32, (nq, ROWS), 0).astype(F32)
    l_row = lax.broadcasted_iota(jnp.int32, (nq, ROWS), 1).astype(F32)
    place = jnp.where(local > 0.5, nq // 2 + ones_before, q_col - ones_before)
    diag = sub128 == lane128
    for j in range(nq // ROWS):
        at = slice(j * ROWS, (j + 1) * ROWS)
        perm_t[:, at] = jnp.where(place == l_row + float(j * ROWS), 1.0, 0.0).astype(BF16)
        row = jnp.sum(jnp.where(diag, place[at, :], 0.0), axis=0, keepdims=True)
        perm[:, at] = jnp.where(row == q_col, 1.0, 0.0).astype(BF16)

    s_lane = lane128.astype(F32)
    par = ranks([select(ids_all[1], gates_all[1], ep_of(k))[0] for k in range(4)])
    pick_par[...] = picks(par)
    for who, r in enumerate((own, par)):
        cols = [jnp.sum(jnp.where(diag, r[k:k + 1, :], 0.0), axis=1, keepdims=True) for k in range(4)]
        for j in range(2):
            hit = jnp.where(s_lane < float(SLOTS), cols[2 * j] - s_lane,
                            cols[2 * j + 1] - s_lane + float(SLOTS)) == 0.0
            merge[who, :, j * ROWS:(j + 1) * ROWS] = jnp.where(hit, 1.0, 0.0).astype(BF16)

    half = nq // 2

    def arrive(kc):
        slot = lax.rem(kc, WRING)
        xs[...] = f32dot(perm[...], slots[kc]).astype(BF16)
        for c in w_copies(kc, slot):
            c.wait()
        return slot

    for kc in range(RELAYS):
        by_way(kc, relay)
        if kc + AHEAD < last:
            by_way(kc + AHEAD, send)

    def k_step(kc, carry):
        later = kc + RELAYS - 1

        by_way(later, relay, (kc >= 1) & (later < RELAYED))
        by_way(later + AHEAD, send, (kc >= 1) & (later + AHEAD < last))

        @pl.when(later == last - 1)
        def _():
            send(last, "direct")

        by_way(kc, take)
        slot = arrive(kc)
        for e in range(2):
            xe = xs[e * half:(e + 1) * half, :]
            for n0, n in chunks(ff, MC):
                at = slice(n0, n0 + n)
                acc_g[e, at, :] += ntdot(wg_buf[slot, e, at, :], xe)
                acc_u[e, at, :] += ntdot(wu_buf[slot, e, at, :], xe)

        @pl.when(kc + WRING < nk)
        def _():
            for c in w_copies(kc + WRING, slot):
                c.start()

        return carry

    lax.fori_loop(0, last, k_step, 0)
    by_way(last, take)
    slot = arrive(last)
    for e in range(2):
        xe = xs[e * half:(e + 1) * half, :]
        for n0, n in chunks(ff, 256):
            at = slice(n0, n0 + n)
            a = acc_g[e, at, :] + ntdot(wg_buf[slot, e, at, :], xe)
            b = acc_u[e, at, :] + ntdot(wu_buf[slot, e, at, :], xe)
            act = (a * (1.0 / (1.0 + jnp.exp(-a))) * b).astype(BF16)
            h[e, :, at] = act.T

    hc = CC // 2

    def a1_copy(s):
        return remote(o_a.at[s, :, 1], a1.at[s], a1_ss.at[s], a1_rs.at[s], 1)

    def a2_copy(s, k):
        return remote(a2s.at[s, k], a2.at[s, k], a2_ss.at[s, k], a2_rs.at[s, k], 2 * k)

    def b1_copy(s, k):
        return remote(o_b.at[s, pl.ds(k * ROWS, ROWS)], b1.at[s, k], b1_ss.at[s, k], b1_rs.at[s, k], 2 * k)

    def b2_copy(s):
        return remote(b2s.at[s], b2.at[s], b2_ss.at[s], b2_rs.at[s], 1)

    def stage1(s):
        slot = lax.rem(s, DRING)
        wd_copy(s, slot).wait()
        for e in range(2):
            parts[e * half:(e + 1) * half, :] = split3(f32dot(h[e], wd_buf[slot, e]))
        for k in range(4):
            at = slice(k * ROWS, (k + 1) * ROWS)
            g = gcol[at, :]
            v = sum3(f32dot(perm_t[at, :], parts[...]))
            va, vb = v[:, :hc] * g, v[:, hc:] * g
            o_a[s, k, 0] = va[:SLOTS]
            o_a[s, k, 1] = va[SLOTS:]
            if k == 0:
                b1[s, 0] = vb
            else:
                o_b[s, at] = vb
        a1_copy(s).start()
        for k in (2, 3, 1):
            b1_copy(s, k).start()

        @pl.when(s + DRING < ns)
        def _():
            wd_copy(s + DRING, slot).start()

    def stage2(s):
        a1_copy(s).wait_recv()
        for k in (2, 3, 1, 0):
            t = o_a[s, k, 0] + a1[s, k]
            if k == 0:
                a2[s, 0] = t
            else:
                a2s[s, k] = t
                a2_copy(s, k).start()
        for k in range(1, 4):
            b1_copy(s, k).wait_recv()
        blocks = b1[s]
        v = blocks[:, SLOTS:, :].reshape(4 * SLOTS, hc)
        b2s[s] = sum3(f32dot(merge[1], split3(v)))
        b2_copy(s).start()
        v = blocks[:, :SLOTS, :].reshape(4 * SLOTS, hc)
        own_b[s] = sum3(f32dot(merge[0], split3(v)))

    def stage3(s):
        for k in range(1, 4):
            a2_copy(s, k).wait_recv()
        v = a2[s].reshape(4 * SLOTS, hc)
        ya = sum3(f32dot(merge[0], split3(v)))
        b2_copy(s).wait_recv()
        yb = own_b[s] + b2[s]
        at = pl.ds(pl.multiple_of(s * CC, CC), CC)
        y_ref[:, at] = jnp.concatenate([ya, yb], axis=1).astype(BF16)

    def s_step(s, carry):
        @pl.when(s < ns)
        def _():
            stage1(s)

        @pl.when((s >= LAG1) & (s < ns + LAG1))
        def _():
            stage2(s - LAG1)

        @pl.when(s >= LAG2)
        def _():
            stage3(s - LAG2)

        return carry

    lax.fori_loop(0, ns + LAG2, s_step, 0)

    def d_done(kc, carry):
        by_way(kc, sent)
        return carry

    lax.fori_loop(0, nk, d_done, 0)

    def s_done(s, carry):
        a1_copy(s).wait_send()
        b2_copy(s).wait_send()
        for k in range(1, 4):
            a2_copy(s, k).wait_send()
            b1_copy(s, k).wait_send()
        return carry

    lax.fori_loop(0, ns, s_done, 0)


def solution(mesh):
    row_spec = P(("dp", "ep", "tp"), None)

    def local_layer(tokens, expert_ids, gates, w_gate, w_up, w_down):
        rows, hidden = tokens.shape
        ff = w_gate.shape[2]
        nk, ns = hidden // KC, hidden // CC
        nq, hc = 8 * SLOTS, CC // 2
        vm, dma = pltpu.VMEM, pltpu.SemaphoreType.DMA
        scratch = [
            vm((8, 2, rows), jnp.int32),
            vm((8, 2, rows), F32),
            vm((nk, 4 * SLOTS, KC), BF16),
            vm((nk // 2, rows, KC), BF16),
            vm((nk // 2, 4 * SLOTS, KC), BF16),
            vm((nk, nq, KC), BF16),
            vm((nq, KC), BF16),
            vm((WRING, 2, ff, KC), BF16),
            vm((WRING, 2, ff, KC), BF16),
            vm((DRING, 2, ff, CC), BF16),
            vm((2, ff, nq // 2), F32),
            vm((2, ff, nq // 2), F32),
            vm((2, nq // 2, ff), BF16),
            vm((4 * SLOTS, rows), BF16),
            vm((nq, nq), BF16),
            vm((nq, nq), BF16),
            vm((2, rows, 4 * SLOTS), BF16),
            vm((nq, ROWS), F32),
            vm((nq, 3 * CC), BF16),
            vm((ns, 4, 2, SLOTS, hc), F32),
            vm((ns, nq, hc), F32),
            vm((ns, 4, SLOTS, hc), F32),
            vm((ns, 4, SLOTS, hc), F32),
            vm((ns, 4, SLOTS, hc), F32),
            vm((ns, 4, ROWS, hc), F32),
            vm((ns, ROWS, hc), F32),
            vm((ns, ROWS, hc), F32),
            vm((ns, ROWS, hc), F32),
            dma((8,)), dma((8,)), dma((8,)), dma((8,)), dma((nk, 8)), dma((nk, 8)), dma((2, WRING)), dma((DRING,)),
            dma((ns,)), dma((ns,)), dma((ns, 4)), dma((ns, 4)),
            dma((ns, 4)), dma((ns, 4)), dma((ns,)), dma((ns,)),
        ]
        vmem = pl.BlockSpec(memory_space=pltpu.VMEM)
        hbm = pl.BlockSpec(memory_space=pl.ANY)
        return pl.pallas_call(
            kernel,
            out_shape=pltpu.VMEM((rows, hidden), BF16),
            in_specs=[vmem, vmem, vmem, hbm, hbm, hbm],
            out_specs=vmem,
            scratch_shapes=scratch,
            compiler_params=pltpu.CompilerParams(
                collective_id=0, has_side_effects=True, vmem_limit_bytes=61_000_000),
        )(expert_ids.T, gates.T, tokens, w_gate.swapaxes(1, 2), w_up.swapaxes(1, 2), w_down)

    return jax.shard_map(
        local_layer, mesh=mesh,
        in_specs=(row_spec, row_spec, row_spec, P("ep", None, "tp"), P("ep", None, "tp"), P("ep", "tp", None)),
        out_specs=row_spec, check_vma=False)
```

```python
import functools

import jax
import jax.numpy as jnp
from jax import lax
from jax.experimental import pallas as pl
from jax.experimental.pallas import tpu as pltpu
from jax.sharding import PartitionSpec as P

MESH = pl.DeviceIdType.MESH
F32 = jnp.float32
BF16 = jnp.bfloat16

ROWS = 128
SLOTS = 64
KC = 256
CC = 256
WRING = 3
WFIRST = 1
MC = 1440
DRING = 2
LAG1, LAG2 = 3, 6
AHEAD = 3
RELAYS = 3
RELAYED = 8


def f32dot(a, b):
    return jnp.dot(a, b, preferred_element_type=F32)


def ntdot(a, b):
    return lax.dot_general(a, b, (((1,), (1,)), ((), ())), preferred_element_type=F32)


def split3(v):
    hi = v.astype(BF16)
    rest = v - hi.astype(F32)
    mid = rest.astype(BF16)
    low = (rest - mid.astype(F32)).astype(BF16)
    return jnp.concatenate([hi, mid, low], axis=1)


def sum3(v):
    n = v.shape[1] // 3
    return (v[:, 2 * n:] + v[:, n:2 * n]) + v[:, :n]


def chunks(total, size):
    return [(i, min(size, total - i)) for i in range(0, total, size)]


def kernel(ids_ref, gates_ref, tok_ref, wg_hbm, wu_hbm, wd_hbm, y_ref,
           ids_all, gates_all, pack, dense, repack, slots, xs, wg_buf, wu_buf, wd_buf, acc_g, acc_u, h,
           pick_par, perm, perm_t, merge, gcol, parts, o_a, o_b,
           a1, a2s, a2, b1, b2s, b2, own_b,
           id_ss, id_rs, gate_ss, gate_rs, d_ss, d_rs, w_sem, wd_sem,
           a1_ss, a1_rs, a2_ss, a2_rs, b1_ss, b1_rs, b2_ss, b2_rs):
    ep, tp = lax.axis_index("ep"), lax.axis_index("tp")
    core, x = lax.rem(ep, 2), lax.div(ep, 2)
    nk, ns = slots.shape[0], o_b.shape[0]
    ff = wg_buf.shape[2]

    def peer(rel):
        dx, dc, dy = rel // 4, (rel // 2) % 2, rel % 2
        return {"ep": lax.rem(x + dx, 2) * 2 + lax.rem(core + dc, 2), "tp": lax.rem(tp + dy, 2)}

    def ep_of(k):
        return lax.rem(x + k // 2, 2) * 2 + lax.rem(core + k % 2, 2)

    def w_copies(kc, slot):
        at = pl.ds(pl.multiple_of(kc * KC, KC), KC)
        return (pltpu.make_async_copy(wg_hbm.at[:, :, at], wg_buf.at[slot], w_sem.at[0, slot]),
                pltpu.make_async_copy(wu_hbm.at[:, :, at], wu_buf.at[slot], w_sem.at[1, slot]))

    def wd_copy(s, slot):
        at = pl.ds(pl.multiple_of(s * CC, CC), CC)
        return pltpu.make_async_copy(wd_hbm.at[:, :, at], wd_buf.at[slot], wd_sem.at[slot])

    def remote(src, dst, ss, rs, rel):
        return pltpu.make_async_remote_copy(src_ref=src, dst_ref=dst, send_sem=ss, recv_sem=rs,
                                            device_id=peer(rel), device_id_type=MESH)

    barrier = pltpu.get_barrier_semaphore()
    for rel in range(1, 8):
        pl.semaphore_signal(barrier, inc=1, device_id=peer(rel), device_id_type=MESH)
    for i in range(WFIRST):
        for c in w_copies(i, i):
            c.start()

    def meta_copies(rel):
        return (remote(ids_ref, ids_all.at[rel], id_ss.at[rel], id_rs.at[rel], rel),
                remote(gates_ref, gates_all.at[rel], gate_ss.at[rel], gate_rs.at[rel], rel))


    sub128 = lax.broadcasted_iota(jnp.int32, (ROWS, ROWS), 0)
    lane128 = lax.broadcasted_iota(jnp.int32, (ROWS, ROWS), 1)
    before = jnp.where(sub128 < lane128, 1.0, 0.0).astype(BF16)

    def select(ids, gates, epv):
        lo = 2.0 * epv.astype(F32)
        ids = ids.astype(F32)
        id0, id1, g0, g1 = ids[0:1, :], ids[1:2, :], gates[0:1, :], gates[1:2, :]
        first = (id0 >= lo) & (id0 <= lo + 1.0)
        second = (id1 >= lo) & (id1 <= lo + 1.0)
        mask = jnp.where(first | second, 1.0, 0.0)
        local = jnp.where(first, id0 - lo, jnp.where(second, id1 - lo, 0.0))
        gate = jnp.where(first, g0, jnp.where(second, g1, 0.0))
        return mask, local, gate

    def ranks(masks):
        m = jnp.concatenate(masks + masks[:1] * (8 - len(masks)), axis=0)
        r = f32dot(m.astype(BF16), before)
        return jnp.where(m > 0.5, r, -1.0)

    slot_iota = lax.broadcasted_iota(jnp.int32, (SLOTS, ROWS), 0).astype(F32)
    own = ranks([select(ids_ref[...], gates_ref[...], ep_of(k))[0] for k in range(4)])

    def picks(r):
        return jnp.concatenate(
            [jnp.where(r[k:k + 1, :] == slot_iota, 1.0, 0.0) for k in range(4)], axis=0).astype(BF16)

    pick = picks(own)

    def d_copy(kc, block, src, to):
        return remote(src, slots.at[kc, pl.ds(block * SLOTS, SLOTS)],
                      d_ss.at[kc, block], d_rs.at[kc, block], to)

    def packed(kc, rel):
        return d_copy(kc, rel, pack.at[kc, pl.ds(rel // 2 * SLOTS, SLOTS)], rel)

    def handed(kc, block):
        return d_copy(kc, block, slots.at[kc, pl.ds((block - 1) * SLOTS, SLOTS)], 1)

    def repacked(kc, block):
        return d_copy(kc, block, repack.at[lax.div(kc, 2), pl.ds(block // 2 * SLOTS, SLOTS)], block - 1)

    def dense_copy(kc):
        at = pl.ds(pl.multiple_of(kc * KC, KC), KC)
        return remote(tok_ref.at[:, at], dense.at[lax.div(kc, 2)], d_ss.at[kc, 1], d_rs.at[kc, 1], 1)

    def send(kc, way):
        if way == "y":
            dense_copy(kc).start()
        for rel in {"x": (4, 6, 1, 3, 2), "y": (4, 6, 2), "direct": (4, 6, 1, 3, 2), "rest": (7, 5)}[way]:
            packed(kc, rel).start()

    def relay(kc, way):
        if way == "x":
            for block in (5, 7):
                packed(kc, block - 1).wait_recv()
                handed(kc, block).start()
        if way == "y":
            dense_copy(kc).wait_recv()
            j = lax.div(kc, 2)
            repack[j] = f32dot(pick_par[...], dense[j]).astype(BF16)
            slots[kc, SLOTS:2 * SLOTS] = repack[j, 0:SLOTS]
            for block in (5, 7, 3):
                repacked(kc, block).start()

    def take(kc, way):
        for block in {"x": (1, 2, 3, 5, 7), "y": (2, 3, 4, 5, 6, 7), "direct": range(1, 8)}[way]:
            packed(kc, block).wait_recv()

    def sent(kc, way):
        if way == "y":
            dense_copy(kc).wait_send()
        for block in range(2 if way == "y" else 1, 8):
            packed(kc, block).wait_send()

    last = nk - 1

    def way_of(kc):
        return "xy"[kc % 2] if kc < RELAYED else "direct"

    def by_way(kc, act, ok=True):
        if isinstance(kc, int):
            act(kc, way_of(kc))
            return
        for i, way in enumerate(("x", "y")):
            @pl.when((lax.rem(kc, 2) == i) & (kc < RELAYED) & ok)
            def _():
                act(kc, way)

        @pl.when((kc >= RELAYED) & ok)
        def _():
            act(kc, "direct")

    for kc in range(nk):
        pack[kc] = f32dot(pick, tok_ref[:, kc * KC:(kc + 1) * KC]).astype(BF16)
        slots[kc, 0:SLOTS] = pack[kc, 0:SLOTS]
    pl.semaphore_wait(barrier, 7)
    for rel in range(1, 8):
        for c in meta_copies(rel):
            c.start()
    for kc in range(AHEAD):
        by_way(kc, send)
    for i in range(WFIRST, WRING):
        for c in w_copies(i, i):
            c.start()
    for i in range(DRING):
        wd_copy(i, i).start()

    acc_g[...] = jnp.zeros_like(acc_g)
    acc_u[...] = jnp.zeros_like(acc_u)

    for rel in range(1, 8):
        for c in meta_copies(rel):
            c.wait()
    ids_all[0] = ids_ref[...]
    gates_all[0] = gates_ref[...]

    chosen = [select(ids_all[rel], gates_all[rel], ep) for rel in range(8)]
    rank_in = ranks([c[0] for c in chosen])
    local_cols = []
    for rel in range(8):
        hit = rank_in[rel:rel + 1, :] == slot_iota
        local_cols.append(jnp.sum(jnp.where(hit, chosen[rel][1], 0.0), axis=1, keepdims=True))
        gcol[rel * SLOTS:(rel + 1) * SLOTS, :] = jnp.broadcast_to(
            jnp.sum(jnp.where(hit, chosen[rel][2], 0.0), axis=1, keepdims=True), (SLOTS, ROWS))
    nq = 8 * SLOTS
    local = jnp.concatenate([jnp.broadcast_to(c, (SLOTS, ROWS)) for c in local_cols], axis=0)
    q_sub = lax.broadcasted_iota(jnp.int32, (nq, nq), 0)
    q_lane = lax.broadcasted_iota(jnp.int32, (nq, nq), 1)
    after = jnp.where(q_sub > q_lane, 1.0, 0.0).astype(BF16)
    ones_before = f32dot(after, local.astype(BF16))
    q_col = lax.broadcasted_iota(jnp.int32, (nq, ROWS), 0).astype(F32)
    l_row = lax.broadcasted_iota(jnp.int32, (nq, ROWS), 1).astype(F32)
    place = jnp.where(local > 0.5, nq // 2 + ones_before, q_col - ones_before)
    diag = sub128 == lane128
    for j in range(nq // ROWS):
        at = slice(j * ROWS, (j + 1) * ROWS)
        perm_t[:, at] = jnp.where(place == l_row + float(j * ROWS), 1.0, 0.0).astype(BF16)
        row = jnp.sum(jnp.where(diag, place[at, :], 0.0), axis=0, keepdims=True)
        perm[:, at] = jnp.where(row == q_col, 1.0, 0.0).astype(BF16)

    s_lane = lane128.astype(F32)
    par = ranks([select(ids_all[1], gates_all[1], ep_of(k))[0] for k in range(4)])
    pick_par[...] = picks(par)
    for who, r in enumerate((own, par)):
        cols = [jnp.sum(jnp.where(diag, r[k:k + 1, :], 0.0), axis=1, keepdims=True) for k in range(4)]
        for j in range(2):
            hit = jnp.where(s_lane < float(SLOTS), cols[2 * j] - s_lane,
                            cols[2 * j + 1] - s_lane + float(SLOTS)) == 0.0
            merge[who, :, j * ROWS:(j + 1) * ROWS] = jnp.where(hit, 1.0, 0.0).astype(BF16)

    half = nq // 2

    def arrive(kc):
        slot = lax.rem(kc, WRING)
        xs[...] = f32dot(perm[...], slots[kc]).astype(BF16)
        for c in w_copies(kc, slot):
            c.wait()
        return slot

    for kc in range(RELAYS):
        by_way(kc, relay)
        if kc + AHEAD < last:
            by_way(kc + AHEAD, send)

    def k_step(kc, carry):
        later = kc + RELAYS - 1

        by_way(later, relay, (kc >= 1) & (later < RELAYED))
        by_way(later + AHEAD, send, (kc >= 1) & (later + AHEAD < last))

        @pl.when(later == last - 2)
        def _():
            send(last, "direct")

        @pl.when(later == last - 1)
        def _():
            send(last, "rest")

        by_way(kc, take)
        slot = arrive(kc)
        for e in range(2):
            xe = xs[e * half:(e + 1) * half, :]
            for n0, n in chunks(ff, MC):
                at = slice(n0, n0 + n)
                acc_g[e, at, :] += ntdot(wg_buf[slot, e, at, :], xe)
                acc_u[e, at, :] += ntdot(wu_buf[slot, e, at, :], xe)

        @pl.when(kc + WRING < nk)
        def _():
            for c in w_copies(kc + WRING, slot):
                c.start()

        return carry

    lax.fori_loop(0, last, k_step, 0)
    by_way(last, take)
    slot = arrive(last)
    for e in range(2):
        xe = xs[e * half:(e + 1) * half, :]
        for n0, n in chunks(ff, 256):
            at = slice(n0, n0 + n)
            a = acc_g[e, at, :] + ntdot(wg_buf[slot, e, at, :], xe)
            b = acc_u[e, at, :] + ntdot(wu_buf[slot, e, at, :], xe)
            act = (a * (1.0 / (1.0 + jnp.exp(-a))) * b).astype(BF16)
            h[e, :, at] = act.T

    hc = CC // 2

    def a1_copy(s):
        return remote(o_a.at[s, :, 1], a1.at[s], a1_ss.at[s], a1_rs.at[s], 1)

    def a2_copy(s, k):
        return remote(a2s.at[s, k], a2.at[s, k], a2_ss.at[s, k], a2_rs.at[s, k], 2 * k)

    def b1_copy(s, k):
        return remote(o_b.at[s, pl.ds(k * ROWS, ROWS)], b1.at[s, k], b1_ss.at[s, k], b1_rs.at[s, k], 2 * k)

    def b2_copy(s):
        return remote(b2s.at[s], b2.at[s], b2_ss.at[s], b2_rs.at[s], 1)

    def stage1(s):
        slot = lax.rem(s, DRING)
        wd_copy(s, slot).wait()
        for e in range(2):
            parts[e * half:(e + 1) * half, :] = split3(f32dot(h[e], wd_buf[slot, e]))
        for k in range(4):
            at = slice(k * ROWS, (k + 1) * ROWS)
            g = gcol[at, :]
            v = sum3(f32dot(perm_t[at, :], parts[...]))
            va, vb = v[:, :hc] * g, v[:, hc:] * g
            o_a[s, k, 0] = va[:SLOTS]
            o_a[s, k, 1] = va[SLOTS:]
            if k == 0:
                b1[s, 0] = vb
            else:
                o_b[s, at] = vb
        a1_copy(s).start()
        for k in (2, 3, 1):
            b1_copy(s, k).start()

        @pl.when(s + DRING < ns)
        def _():
            wd_copy(s + DRING, slot).start()

    def stage2(s):
        a1_copy(s).wait_recv()
        for k in (2, 3, 1, 0):
            t = o_a[s, k, 0] + a1[s, k]
            if k == 0:
                a2[s, 0] = t
            else:
                a2s[s, k] = t
                a2_copy(s, k).start()
        for k in range(1, 4):
            b1_copy(s, k).wait_recv()
        blocks = b1[s]
        v = blocks[:, SLOTS:, :].reshape(4 * SLOTS, hc)
        b2s[s] = sum3(f32dot(merge[1], split3(v)))
        b2_copy(s).start()
        v = blocks[:, :SLOTS, :].reshape(4 * SLOTS, hc)
        own_b[s] = sum3(f32dot(merge[0], split3(v)))

    def stage3(s):
        for k in range(1, 4):
            a2_copy(s, k).wait_recv()
        v = a2[s].reshape(4 * SLOTS, hc)
        ya = sum3(f32dot(merge[0], split3(v)))
        b2_copy(s).wait_recv()
        yb = own_b[s] + b2[s]
        at = pl.ds(pl.multiple_of(s * CC, CC), CC)
        y_ref[:, at] = jnp.concatenate([ya, yb], axis=1).astype(BF16)

    def s_step(s, carry):
        @pl.when(s < ns)
        def _():
            stage1(s)

        @pl.when((s >= LAG1) & (s < ns + LAG1))
        def _():
            stage2(s - LAG1)

        @pl.when(s >= LAG2)
        def _():
            stage3(s - LAG2)

        return carry

    lax.fori_loop(0, ns + LAG2, s_step, 0)

    def d_done(kc, carry):
        by_way(kc, sent)
        return carry

    lax.fori_loop(0, nk, d_done, 0)

    def s_done(s, carry):
        a1_copy(s).wait_send()
        b2_copy(s).wait_send()
        for k in range(1, 4):
            a2_copy(s, k).wait_send()
            b1_copy(s, k).wait_send()
        return carry

    lax.fori_loop(0, ns, s_done, 0)


def solution(mesh):
    row_spec = P(("dp", "ep", "tp"), None)

    def local_layer(tokens, expert_ids, gates, w_gate, w_up, w_down):
        rows, hidden = tokens.shape
        ff = w_gate.shape[2]
        nk, ns = hidden // KC, hidden // CC
        nq, hc = 8 * SLOTS, CC // 2
        vm, dma = pltpu.VMEM, pltpu.SemaphoreType.DMA
        scratch = [
            vm((8, 2, rows), jnp.int32),
            vm((8, 2, rows), F32),
            vm((nk, 4 * SLOTS, KC), BF16),
            vm((nk // 2, rows, KC), BF16),
            vm((nk // 2, 4 * SLOTS, KC), BF16),
            vm((nk, nq, KC), BF16),
            vm((nq, KC), BF16),
            vm((WRING, 2, ff, KC), BF16),
            vm((WRING, 2, ff, KC), BF16),
            vm((DRING, 2, ff, CC), BF16),
            vm((2, ff, nq // 2), F32),
            vm((2, ff, nq // 2), F32),
            vm((2, nq // 2, ff), BF16),
            vm((4 * SLOTS, rows), BF16),
            vm((nq, nq), BF16),
            vm((nq, nq), BF16),
            vm((2, rows, 4 * SLOTS), BF16),
            vm((nq, ROWS), F32),
            vm((nq, 3 * CC), BF16),
            vm((ns, 4, 2, SLOTS, hc), F32),
            vm((ns, nq, hc), F32),
            vm((ns, 4, SLOTS, hc), F32),
            vm((ns, 4, SLOTS, hc), F32),
            vm((ns, 4, SLOTS, hc), F32),
            vm((ns, 4, ROWS, hc), F32),
            vm((ns, ROWS, hc), F32),
            vm((ns, ROWS, hc), F32),
            vm((ns, ROWS, hc), F32),
            dma((8,)), dma((8,)), dma((8,)), dma((8,)), dma((nk, 8)), dma((nk, 8)), dma((2, WRING)), dma((DRING,)),
            dma((ns,)), dma((ns,)), dma((ns, 4)), dma((ns, 4)),
            dma((ns, 4)), dma((ns, 4)), dma((ns,)), dma((ns,)),
        ]
        vmem = pl.BlockSpec(memory_space=pltpu.VMEM)
        hbm = pl.BlockSpec(memory_space=pl.ANY)
        return pl.pallas_call(
            kernel,
            out_shape=pltpu.VMEM((rows, hidden), BF16),
            in_specs=[vmem, vmem, vmem, hbm, hbm, hbm],
            out_specs=vmem,
            scratch_shapes=scratch,
            compiler_params=pltpu.CompilerParams(
                collective_id=0, has_side_effects=True, vmem_limit_bytes=61_000_000),
        )(expert_ids.T, gates.T, tokens, w_gate.swapaxes(1, 2), w_up.swapaxes(1, 2), w_down)

    return jax.shard_map(
        local_layer, mesh=mesh,
        in_specs=(row_spec, row_spec, row_spec, P("ep", None, "tp"), P("ep", None, "tp"), P("ep", "tp", None)),
        out_specs=row_spec, check_vma=False)
```
